32 devices in a mesh: vec: 16 (over z, y, x), ao: 2 (over core).
Axes of the slice: x: 2, y: 2, z: 4, core: 2. Of those that a mesh axis runs over, the one named last changes fastest.
Arguments:
- cholesky: float32 [16, 1200, 1200], P('vec', 'ao'), may hold values from -6 to 6
- coefficients: float32 [2, 720000], P('ao', 'vec'), may hold values from -0.1875 to 0.1875
Outputs:
- mo_vectors: float32 [16, 128, 1072], P(None, 'vec', 'ao')
The draws below stay inside these ranges and needn't reach their ends.
All inputs are finite; a program needn't handle non-finite values.
Results may differ from the reference program's by a relative error of at most 0.0001.
Values sent between devices are 32-bit elements; how exact they have to be, the bound alone decides.
A program may use at most 64 MiB of HBM per device.

```python
import jax
import jax.numpy as jnp
from jax import lax

NAO = 1200
NOCC = 128
NVIR = 1072
NMO = 1200
HALF_AO = 600
NVEC = 16
N_AO = 2


def steps_of(key, shape, split, low, top_value):
    level, own = 1.0, jax.random.fold_in(key, 6)
    for position, blocks in split:
        steps = jnp.exp(jax.random.uniform(jax.random.fold_in(own, position), (blocks,), jnp.float32, low / len(split), top_value / len(split)))
        level = level * jnp.repeat(steps, shape[position] // blocks).reshape([-1 if axis == position else 1 for axis in range(len(shape))])
    return level


def bell_draw(stream_key, extent, width, most, split=(), kind=jnp.bfloat16):
    entries = width * jax.random.normal(stream_key, extent, jnp.float32)
    if split:
        entries = entries * steps_of(stream_key, extent, split, -0.22, 0.18)
    return jnp.clip(entries, -most, most).astype(kind)


def setup_inputs(seed: int = 0) -> dict:
    streams_of = jax.random.split(jax.random.key(seed), 3)
    cholesky = bell_draw(streams_of[0], (NVEC, NAO, NAO), 1.0, 6.0, ((0, 16), (1, 2)), jnp.float32)
    coefficients = bell_draw(streams_of[1], (N_AO, HALF_AO * NMO), NAO ** -0.5, 0.1875, ((0, 2), (1, 16)), jnp.float32)
    return dict(cholesky=cholesky, coefficients=coefficients)


def reference(cholesky, coefficients):
    matrix = coefficients.reshape(NAO, NOCC + NVIR)
    occupied = matrix[:, :NOCC]
    virtual = matrix[:, NOCC:]

    def transform_one(vector):
        left_half = jnp.dot(occupied.T, vector, precision=lax.Precision.HIGHEST, preferred_element_type=jnp.float32)
        return jnp.dot(left_half, virtual, precision=lax.Precision.HIGHEST, preferred_element_type=jnp.float32)

    return lax.map(transform_one, cholesky)
```

```python
import functools
import math

import jax
import jax.numpy as jnp
from jax import lax
from jax.experimental import pallas as pl
from jax.experimental.pallas import tpu as pltpu
from jax.sharding import PartitionSpec as P

NOCC = 128
LANES = 128
MESH = pl.DeviceIdType.MESH
F32 = jnp.float32
BF16 = jnp.bfloat16


def up_to(size, step):
    return -(-size // step) * step


def simple_body(cholesky, coefficients):
    half_rows = cholesky.shape[1]
    own_flat = lax.all_gather(coefficients, "vec", axis=1, tiled=True)
    own_rows = own_flat.reshape(half_rows, own_flat.shape[1] // half_rows)
    occupied_own = own_rows[:, :NOCC]
    partial_x = jnp.einsum(
        "mi,pmn->pin",
        occupied_own,
        cholesky,
        precision=lax.Precision.HIGHEST,
        preferred_element_type=jnp.float32,
    )
    x_block = lax.psum_scatter(partial_x, "ao", scatter_dimension=2, tiled=True)
    virtual_own = own_rows[:, NOCC:]
    partial_y = jnp.einsum(
        "pin,na->pia",
        x_block,
        virtual_own,
        precision=lax.Precision.HIGHEST,
        preferred_element_type=jnp.float32,
    )
    summed = lax.psum_scatter(partial_y, "ao", scatter_dimension=2, tiled=True)
    owned = lax.all_to_all(summed, "vec", split_axis=1, concat_axis=0, tiled=True)
    return owned


def split(value):
    high = value.astype(BF16)
    return high, (value - high.astype(F32)).astype(BF16)


def product(left, right):
    (lh, ll), (rh, rl) = left, right
    dot = functools.partial(jnp.dot, preferred_element_type=F32)
    return dot(lh, rh) + (dot(lh, rl) + dot(ll, rh))


def tile_at(tiles, lane, offset):
    first, shift = divmod(offset, LANES)
    blank = jnp.zeros_like(tiles[0])
    here, after = (tiles[k] if 0 <= k < len(tiles) else blank for k in (first, first + 1))
    if shift == 0:
        return here
    turn = LANES - shift
    return jnp.where(lane < turn, pltpu.roll(here, turn, 1), pltpu.roll(after, turn, 1))


def kernel(
    n, starts, rows, deep, parts, sub_ref, l_ref, out_ref,
    sbuf, occ_all, vsend, va, l_buf, lh, ll, occ_dense, dense, vh, vl,
    x_out, x_in, x_own, x_send, x_recv, y_out, y_in, y_send, y_recv,
    l_sem, occ_zs, occ_ss, occ_rs, vx_ss, v_ss, v_rs, x_ss, xf_ss, x_rs, pair_ss, pair_rs, y_ss, y_rs, o_ss, o_rs,
):
    me, core = lax.axis_index("vec"), lax.axis_index("ao")
    nz = n // 4
    x, y, z = me % 2, (me // 2) % 2, me // 4
    xp, yp, diag = me + 1 - 2 * x, me + 2 - 4 * y, me + 3 - 2 * x - 4 * y
    half, nao = l_ref.shape
    subs, sub = sub_ref.shape
    wide = out_ref.shape[2]
    full = wide // LANES
    rest = wide - full * LANES
    groups = deep // 8
    body_rows = full * deep
    block = 2 * out_ref.shape[1]
    npair = n // 2
    mine = me // 2

    l_copy = pltpu.make_async_copy(l_ref, l_buf, l_sem)
    l_copy.start()

    barrier = pltpu.get_barrier_semaphore()
    for to in [(me + 4 * d) % n for d in range(1, nz)] + [xp, yp, diag]:
        pl.semaphore_signal(barrier, inc=1, device_id=(to, core), device_id_type=MESH)
    pl.semaphore_signal(barrier, inc=1, device_id=(me, 1 - core), device_id_type=MESH)

    sbuf[...] = jnp.zeros_like(sbuf)
    for t in range(sbuf.shape[0]):
        width = min(LANES, sub - t * LANES)
        sbuf[t, 8:8 + subs, :width] = sub_ref[:, t * LANES:t * LANES + width]
    lane = lax.broadcasted_iota(jnp.int32, (deep, LANES), 1)
    odd = (me * subs) % 2 == 1
    left, right = [], []
    for t in range(sbuf.shape[0]):
        before, even, after = (sbuf[t, pl.ds(8 + k, deep, stride=2), :] for k in (-1, 0, 1))
        left.append(jnp.where(odd, before, even))
        right.append(jnp.where(odd, even, after))
    columns = []
    for t in range(up_to(2 * sub, LANES) // LANES):
        value = tile_at(right, lane, t * LANES - sub)
        columns.append(value + left[t] if t < len(left) else value)
    occ_all[me] = columns[0]
    halves = [[tile_at(columns, lane, NOCC + h * wide + t * LANES) for t in range(full + 1)] for h in range(2)]
    tails = []
    for h in range(2):
        tail = jnp.zeros((8, LANES), F32)
        for g in range(groups):
            piece = jnp.where(lane[:8] < rest, halves[h][full][8 * g:8 * g + 8], 0)
            tail += pltpu.roll(piece, g * rest, 1) if g else piece
        tails.append(tail)
    for t in range(full):
        low, high = halves[0][t], halves[1][t]
        va[me, t * deep:(t + 1) * deep, :] = jnp.where(x == 0, low, high)
        vsend[t * deep:(t + 1) * deep, :] = jnp.where(x == 0, high, low)
    va[me, body_rows:body_rows + 8, :] = jnp.where(x == 0, tails[0], tails[1])
    vsend[body_rows:body_rows + 8, :] = jnp.where(x == 0, tails[1], tails[0])

    pl.semaphore_wait(barrier, nz + 3)

    def remote(src, dst, send_sem, recv_sem, to, on=core):
        return pltpu.make_async_remote_copy(
            src_ref=src, dst_ref=dst, send_sem=send_sem, recv_sem=recv_sem,
            device_id=(to, on), device_id_type=MESH)

    def occ_line_copy(w, d, to):
        return remote(occ_all.at[w], occ_all.at[w], occ_zs.at[d], occ_rs.at[w], to)

    def occ_copy(w, way, to):
        return remote(occ_all.at[w], occ_all.at[w], occ_ss.at[way, w], occ_rs.at[w], to)

    def half_copy(p, w, to):
        rng = pl.ds(parts[p][0], parts[p][1])
        return remote(vsend.at[rng], va.at[w, rng], vx_ss.at[p], v_rs.at[p, w], to)

    def vir_copy(p, w, way, to):
        ref = va.at[w, pl.ds(parts[p][0], parts[p][1])]
        return remote(ref, ref, v_ss.at[way, p, w], v_rs.at[p, w], to)

    def x_copy(q, w, d, to):
        return remote(x_send.at[q], x_recv.at[w], x_ss.at[d], x_rs.at[w], to)

    def x_pass(w, to):
        return remote(x_recv.at[w], x_recv.at[w], xf_ss.at[w], x_rs.at[w], to)

    def pair_copy():
        return remote(x_out, x_in, pair_ss, pair_rs, me, 1 - core)

    def y_copy(k, group):
        return remote(y_out.at[group], y_in.at[group], y_ss.at[k], y_rs.at[k], me, 1 - core)

    def o_copy(k, group):
        return remote(y_send.at[group], y_recv.at[group], o_ss.at[k], o_rs.at[k], xp, 1 - core)

    def signs(k, act):
        if 0 < k < nz:
            pl.when(z >= k)(lambda: act(-4 * k, True))
            pl.when(z + k < nz)(lambda: act(4 * k, False))

    def along(p, w, up=True, down=True):
        if up:
            pl.when(z < nz - 1)(lambda: vir_copy(p, w, 1, me + 4).start())
        if down:
            pl.when(z > 0)(lambda: vir_copy(p, w, 2, me - 4).start())

    def occ_spread(w):
        for way, to in enumerate((xp, yp, diag)):
            occ_copy(w, way, to).start()

    def occ_start():
        for d in range(1, nz):
            occ_line_copy(me, d, (me + 4 * d) % n).start()
        occ_spread(me)

    def occ_line():
        for k in range(1, nz):
            def act(offset, up):
                occ_copy(me + offset, 0, me).wait_recv()
                occ_spread(me + offset)
            signs(k, act)

    def own_start():
        for p in range(len(parts)):
            half_copy(p, me, xp).start()
            along(p, me)
            vir_copy(p, me, 0, yp).start()

    def prepare():
        dense[...] = jnp.zeros_like(dense)
        occ_dense[...] = jnp.zeros_like(occ_dense)
        edge = half // LANES * LANES
        lh[:, :, edge:] = jnp.zeros_like(lh[:, :, edge:])
        ll[:, :, edge:] = jnp.zeros_like(ll[:, :, edge:])
        l_copy.wait()
        for h in range(2):
            high, low = split(l_buf[:, h * half:(h + 1) * half])
            lh[h, :, :half] = high
            ll[h, :, :half] = low

    def cross(p):
        half_copy(p, xp, me).wait_recv()
        along(p, xp)
        vir_copy(p, xp, 0, yp).start()

    def line(k, p, column):
        def act(offset, up):
            w = (me if column == 0 else xp) + offset
            vir_copy(p, w, 1, me).wait_recv()
            along(p, w, up, not up)
            vir_copy(p, w, 0, yp).start()
        signs(k, act)

    def half_transform():
        for d in range(nz):
            for other in (xp, yp, diag):
                occ_copy((other + 4 * d) % n, 0, me).wait_recv()
        for w in range(n):
            occ_dense[starts[w]:starts[w] + rows, :] += occ_all[w, :rows, :]
        occ = split(occ_dense[...].T[:, :half])
        x_out[...] = product(occ, (lh[1 - core], ll[1 - core]))
        pair_copy().start()
        x_own[...] = product(occ, (lh[core], ll[core]))

    def x_start():
        pair_copy().wait_recv()
        x_send[...] = (x_own[...] + x_in[...]).reshape(x_send.shape)
        x_copy(mine, me, 0, xp).start()
        for d in range(1, npair):
            q = (mine + d) % npair
            x_copy(q, me, d, 2 * q + x).start()
        x_recv[me] = x_send[mine]

    def x_take(w):
        x_copy(mine, w, 0, me).wait_recv()
        x_pass(w, xp).start()

    def x_relay(k):
        if k == 0:
            x_take(yp)
        else:
            def act(offset, up):
                x_take(me + offset)
                x_take(yp + offset)
            signs(k, act)

    def y_wait():
        for p in range(len(parts)):
            for zz in range(nz):
                for other in (yp, diag):
                    vir_copy(p, (other + 4 * zz) % n, 0, me).wait_recv()

    def join():
        tlane = lane
        for w in range(n):
            top = starts[w]
            for t in range(full):
                dense[top:top + rows, t * LANES:(t + 1) * LANES] += va[w, t * deep:t * deep + rows, :]
            tail = va[w, body_rows:body_rows + 8, :]
            value = jnp.concatenate([pltpu.roll(tail, (LANES - g * rest) % LANES, 1) if g else tail for g in range(groups)], axis=0)
            value = jnp.where(tlane < rest, value, 0)
            dense[top:top + rows, full * LANES:(full + 1) * LANES] += value[:rows]
        high, low = split(dense[...])
        vh[...] = high
        vl[...] = low

    def plane_of(k):
        order = [sorted(range(nz), key=lambda other: (abs(other - zz), other)) for zz in range(nz)]
        which = 0
        for zz in range(nz):
            which = which + jnp.where(z == zz, order[zz][k], 0)
        return which

    far = core != x

    def chunk(k):
        plane = plane_of(k)
        group = pl.ds(4 * plane, 4)
        for j in range(4):
            w = 4 * plane + j

            @pl.when((w % 2 != x))
            def _():
                x_pass(w, me).wait_recv()
        tall = 4 * block
        value = product(split(x_recv[group].reshape(tall, x_recv.shape[2])), (vh[...], vl[...]))
        value = value.reshape(4, block, value.shape[1])
        low, high = value[:, :block // 2], value[:, block // 2:]
        y_out[group] = jnp.where(core == 0, high, low)
        y_send[group] = jnp.where(core == 0, low, high)
        y_copy(k, group).start()

    def finish(k):
        group = pl.ds(4 * plane_of(k), 4)
        y_copy(k, group).wait_recv()
        total = y_send[group] + y_in[group]
        y_send[group] = total

        @pl.when(far)
        def _():
            o_copy(k, group).start()

        @pl.when(jnp.logical_not(far))
        def _():
            out_ref[group] = total[:, :, :wide]

    def last(k):
        group = pl.ds(4 * plane_of(k), 4)

        @pl.when(far)
        def _():
            o_copy(k, group).wait_recv()
            out_ref[group] = y_recv[group, :, :wide]

    pieces = range(len(parts))
    occ_start()
    own_start()
    prepare()
    occ_line()
    for p in pieces:
        cross(p)
    for p in pieces:
        line(1, p, 0)
    half_transform()
    for p in pieces:
        line(1, p, 1)
    for p in pieces:
        line(2, p, 0)
    x_start()
    for p in pieces:
        line(2, p, 1)
    for k in range(3, nz):
        for column in range(2):
            for p in pieces:
                line(k, p, column)
    for k in range(nz):
        x_relay(k)
    y_wait()
    join()
    for k in range(nz):
        chunk(k)
        if k:
            finish(k - 1)
    finish(nz - 1)

    for d in range(1, nz):
        occ_line_copy(me, d, me).wait_send()
    for zz in range(nz):
        for way in range(3):
            occ_copy((me + 4 * zz) % n, way, xp).wait_send()
    for p in pieces:
        half_copy(p, me, xp).wait_send()
        for zz in range(nz):
            for base in (me, xp):
                w = base - 4 * z + 4 * zz
                vir_copy(p, w, 0, yp).wait_send()
                pl.when((z >= zz) & (z < nz - 1))(lambda: vir_copy(p, w, 1, yp).wait_send())
                pl.when((z <= zz) & (z > 0))(lambda: vir_copy(p, w, 2, yp).wait_send())
    pair_copy().wait_send()
    for d in range(npair):
        x_copy(mine, me, d, xp).wait_send()
    for d in range(1, npair):
        x_pass(((2 * (mine + d)) % n) + x, xp).wait_send()
    for k in range(nz):
        group = pl.ds(4 * plane_of(k), 4)
        y_copy(k, group).wait_send()
        pl.when(far)(lambda: o_copy(k, group).wait_send())
        last(k)


def body(n, cholesky, coefficients):
    half, nao = cholesky.shape[1:]
    per = coefficients.shape[1]
    nmo = per * n // half
    nvir = nmo - NOCC
    sub = math.gcd(per, nmo)
    wide = nvir // 2
    full, rest = wide // LANES, wide % LANES
    starts = tuple(w * per // nmo for w in range(n))
    rows = max(-(-(w * per % nmo + per) // nmo) for w in range(n))
    deep = up_to(rows, 8)
    if cholesky.shape[0] != 1 or nmo != 2 * sub or rest == 0 or rest * (deep // 8) > LANES:
        return simple_body(cholesky, coefficients)
    subs = per // sub
    tall = up_to(max(half, starts[-1] + rows), LANES)
    size = full * deep + 8
    cut = full // 2 * deep
    parts = ((0, cut), (cut, size - cut))
    iblock = NOCC // n
    spread = up_to(wide, LANES)
    nz = n // 4
    dma = pltpu.SemaphoreType.DMA
    vmem = pl.BlockSpec(memory_space=pltpu.VMEM)
    return pl.pallas_call(
        functools.partial(kernel, n, starts, rows, deep, parts),
        out_shape=jax.ShapeDtypeStruct((n, iblock, wide), F32),
        in_specs=[vmem, pl.BlockSpec(memory_space=pl.ANY)],
        out_specs=vmem,
        scratch_shapes=[
            pltpu.VMEM((up_to(sub, LANES) // LANES, up_to(9 + 2 * deep, 8), LANES), F32),
            pltpu.VMEM((n, deep, LANES), F32),
            pltpu.VMEM((size, LANES), F32),
            pltpu.VMEM((n, size, LANES), F32),
            pltpu.VMEM((half, nao), F32),
            pltpu.VMEM((2, half, tall), BF16),
            pltpu.VMEM((2, half, tall), BF16),
            pltpu.VMEM((tall, NOCC), F32),
            pltpu.VMEM((tall, spread), F32),
            pltpu.VMEM((tall, spread), BF16),
            pltpu.VMEM((tall, spread), BF16),
            pltpu.VMEM((NOCC, tall), F32),
            pltpu.VMEM((NOCC, tall), F32),
            pltpu.VMEM((NOCC, tall), F32),
            pltpu.VMEM((n // 2, 2 * iblock, tall), F32),
            pltpu.VMEM((n, 2 * iblock, tall), F32),
            pltpu.VMEM((n, iblock, spread), F32),
            pltpu.VMEM((n, iblock, spread), F32),
            pltpu.VMEM((n, iblock, spread), F32),
            pltpu.VMEM((n, iblock, spread), F32),
            dma, dma((nz,)), dma((3, n)), dma((n,)), dma((len(parts),)), dma((3, len(parts), n)), dma((len(parts), n)),
            dma((n // 2,)), dma((n,)), dma((n,)), dma, dma, dma((nz,)), dma((nz,)), dma((nz,)), dma((nz,)),
        ],
        compiler_params=pltpu.CompilerParams(
            collective_id=0, has_side_effects=True, vmem_limit_bytes=32 * 1024 * 1024),
        name="transform",
    )(coefficients[0].reshape(subs, sub), cholesky[0])


def solution(mesh):
    n = mesh.shape["vec"]
    in_specs = (P("vec", "ao", None), P("ao", "vec"))
    out_specs = P(None, "vec", "ao")
    lines = n % 4 == 0 and mesh.shape["ao"] == 2 and NOCC % (8 * n) == 0
    step = functools.partial(body, n) if lines else simple_body
    return jax.shard_map(step, mesh=mesh, in_specs=in_specs, out_specs=out_specs, check_vma=False)
```

```python
import functools
import math

import jax
import jax.numpy as jnp
from jax import lax
from jax.experimental import pallas as pl
from jax.experimental.pallas import tpu as pltpu
from jax.sharding import PartitionSpec as P

NOCC = 128
LANES = 128
MESH = pl.DeviceIdType.MESH
F32 = jnp.float32
TURN, TURNED, GROUPS = 1, (1,), 4
BF16 = jnp.bfloat16


def up_to(size, step):
    return -(-size // step) * step


def simple_body(cholesky, coefficients):
    half_rows = cholesky.shape[1]
    own_flat = lax.all_gather(coefficients, "vec", axis=1, tiled=True)
    own_rows = own_flat.reshape(half_rows, own_flat.shape[1] // half_rows)
    occupied_own = own_rows[:, :NOCC]
    partial_x = jnp.einsum(
        "mi,pmn->pin",
        occupied_own,
        cholesky,
        precision=lax.Precision.HIGHEST,
        preferred_element_type=jnp.float32,
    )
    x_block = lax.psum_scatter(partial_x, "ao", scatter_dimension=2, tiled=True)
    virtual_own = own_rows[:, NOCC:]
    partial_y = jnp.einsum(
        "pin,na->pia",
        x_block,
        virtual_own,
        precision=lax.Precision.HIGHEST,
        preferred_element_type=jnp.float32,
    )
    summed = lax.psum_scatter(partial_y, "ao", scatter_dimension=2, tiled=True)
    owned = lax.all_to_all(summed, "vec", split_axis=1, concat_axis=0, tiled=True)
    return owned


def split(value):
    high = value.astype(BF16)
    return high, (value - high.astype(F32)).astype(BF16)


def product(left, right):
    (lh, ll), (rh, rl) = left, right
    dot = functools.partial(jnp.dot, preferred_element_type=F32)
    return dot(lh, rh) + (dot(lh, rl) + dot(ll, rh))


def tile_at(tiles, lane, offset):
    first, shift = divmod(offset, LANES)
    blank = jnp.zeros_like(tiles[0])
    here, after = (tiles[k] if 0 <= k < len(tiles) else blank for k in (first, first + 1))
    if shift == 0:
        return here
    turn = LANES - shift
    return jnp.where(lane < turn, pltpu.roll(here, turn, 1), pltpu.roll(after, turn, 1))


def kernel(
    n, starts, rows, deep, sub, parts, split_at, raw_ref, l_ref, out_ref,
    flat, sbuf, occ_all, vsend, va, l_buf, lh, ll, occ_dense, oh, ol, dense, vh, vl,
    x_out, x_in, x_own, x_send, x_recv, y_out, y_in, y_sum, y_recv,
    l_sem, occ_zs, occ_ss, occ_rs, vx_ss, v_ss, v_rs, x_ss, xf_ss, x_rs, pair_ss, pair_rs, y_ss, y_rs, o_ss, o_rs,
):
    me, core = lax.axis_index("vec"), lax.axis_index("ao")
    nz = n // 4
    x, y, z = me % 2, (me // 2) % 2, me // 4
    xp, yp, diag = me + 1 - 2 * x, me + 2 - 4 * y, me + 3 - 2 * x - 4 * y
    half, nao = l_ref.shape
    per = raw_ref.shape[1]
    subs = per // sub
    wide = out_ref.shape[2]
    full = wide // LANES
    rest = wide - full * LANES
    groups = deep // 8
    body_rows = full * rows
    block = 2 * out_ref.shape[1]
    npair = n // 2
    mine = me // 2

    l_copy = pltpu.make_async_copy(l_ref, l_buf, l_sem)
    l_copy.start()

    barrier = pltpu.get_barrier_semaphore()
    for to in [(me + 4 * d) % n for d in range(1, nz)] + [xp, yp, diag]:
        pl.semaphore_signal(barrier, inc=1, device_id=(to, core), device_id_type=MESH)
    pl.semaphore_signal(barrier, inc=1, device_id=(me, 1 - core), device_id_type=MESH)

    sbuf[...] = jnp.zeros_like(sbuf)
    for k in range(up_to(per, LANES) // LANES):
        width = min(LANES, per - k * LANES)
        flat[k:k + 1, :width] = raw_ref[:, k * LANES:k * LANES + width]
    period = LANES // math.gcd(sub, LANES)
    step = period * sub // LANES
    lane = lax.broadcasted_iota(jnp.int32, (deep, LANES), 1)
    for b in range(min(period, subs)):
        count = -(-(subs - b) // period)
        for t in range(sbuf.shape[0]):
            at, shift = divmod(b * sub + t * LANES, LANES)
            value = flat[pl.ds(at, count, stride=step), :]
            if shift:
                later = flat[pl.ds(at + 1, count, stride=step), :]
                turn = LANES - shift
                value = jnp.where(lane[:count] < turn, pltpu.roll(value, turn, 1), pltpu.roll(later, turn, 1))
            value = jnp.where(lane[:count] < sub - t * LANES, value, 0)
            sbuf[t, pl.ds(8 + b, count, stride=period), :] = value
    odd = (me * subs) % 2 == 1
    left, right = [], []
    for t in range(sbuf.shape[0]):
        before, even, after = (sbuf[t, pl.ds(8 + k, deep, stride=2), :] for k in (-1, 0, 1))
        left.append(jnp.where(odd, before, even))
        right.append(jnp.where(odd, even, after))
    columns = []
    for t in range(up_to(2 * sub, LANES) // LANES):
        value = tile_at(right, lane, t * LANES - sub)
        columns.append(value + left[t] if t < len(left) else value)
    occ_all[me] = columns[0]
    halves = [[tile_at(columns, lane, NOCC + h * wide + t * LANES) for t in range(full + 1)] for h in range(2)]
    tails = []
    for h in range(2):
        tail = jnp.zeros((8, LANES), F32)
        for g in range(groups):
            piece = jnp.where(lane[:8] < rest, halves[h][full][8 * g:8 * g + 8], 0)
            tail += pltpu.roll(piece, g * rest, 1) if g else piece
        tails.append(tail)
    for t in range(full):
        low, high = halves[0][t], halves[1][t]
        va[me, t * rows:(t + 1) * rows, :] = jnp.where(x == 0, low, high)[:rows]
        vsend[t * rows:(t + 1) * rows, :] = jnp.where(x == 0, high, low)[:rows]
    va[me, body_rows:body_rows + 8, :] = jnp.where(x == 0, tails[0], tails[1])
    vsend[body_rows:body_rows + 8, :] = jnp.where(x == 0, tails[1], tails[0])

    pl.semaphore_wait(barrier, nz + 3)

    def remote(src, dst, send_sem, recv_sem, to, on=core):
        return pltpu.make_async_remote_copy(
            src_ref=src, dst_ref=dst, send_sem=send_sem, recv_sem=recv_sem,
            device_id=(to, on), device_id_type=MESH)

    def occ_line_copy(w, d, to):
        return remote(occ_all.at[w], occ_all.at[w], occ_zs.at[d], occ_rs.at[w], to)

    def occ_copy(w, way, to):
        return remote(occ_all.at[w], occ_all.at[w], occ_ss.at[way, w], occ_rs.at[w], to)

    def half_copy(p, w, to):
        rng = pl.ds(parts[p][0], parts[p][1])
        return remote(vsend.at[rng], va.at[w, rng], vx_ss.at[p], v_rs.at[p, w], to)

    def vir_copy(p, w, way, to):
        ref = va.at[w, pl.ds(parts[p][0], parts[p][1])]
        return remote(ref, ref, v_ss.at[way, p, w], v_rs.at[p, w], to)

    def x_copy(q, w, d, to):
        return remote(x_send.at[q], x_recv.at[w], x_ss.at[d], x_rs.at[w], to)

    def x_pass(w, to):
        return remote(x_recv.at[w], x_recv.at[w], xf_ss.at[w], x_rs.at[w], to)

    def pair_copy():
        return remote(x_out, x_in, pair_ss, pair_rs, me, 1 - core)

    def y_copy(w):
        return remote(y_out.at[w], y_in.at[w], y_ss.at[w], y_rs.at[w], me, 1 - core)

    def o_copy(w):
        return remote(y_sum.at[w], y_recv.at[w], o_ss.at[w], o_rs.at[w], xp, 1 - core)

    state = dict(end=False)

    def start(copy):
        copy.wait_send() if state["end"] else copy.start()

    def recv(copy, *where):
        if not state["end"]:
            copy(*where).wait_recv()

    def signs(k, act):
        if 0 < k < nz:
            pl.when(z >= k)(lambda: act(-4 * k, True))
            pl.when(z + k < nz)(lambda: act(4 * k, False))

    def along(p, w, up=True, down=True):
        if up:
            pl.when(z < nz - 1)(lambda: start(vir_copy(p, w, 1, me + 4)))
        if down:
            pl.when(z > 0)(lambda: start(vir_copy(p, w, 2, me - 4)))

    def occ_spread(w):
        for way, to in enumerate((xp, yp, diag)):
            start(occ_copy(w, way, to))

    def occ_start():
        for d in range(1, nz):
            start(occ_line_copy(me, d, (me + 4 * d) % n))
        occ_spread(me)

    def occ_line():
        for k in range(1, nz):
            def act(offset, up):
                recv(occ_copy, me + offset, 0, me)
                occ_spread(me + offset)
            signs(k, act)

    def own_start(p):
        start(half_copy(p, me, xp))
        along(p, me)
        start(vir_copy(p, me, 0, yp))

    def prepare():
        dense[...] = jnp.zeros_like(dense)
        occ_dense[...] = jnp.zeros_like(occ_dense)
        edge = half // LANES * LANES
        lh[:, :, edge:] = jnp.zeros_like(lh[:, :, edge:])
        ll[:, :, edge:] = jnp.zeros_like(ll[:, :, edge:])
        l_copy.wait()
        for h in range(2):
            high, low = split(l_buf[:, h * half:(h + 1) * half])
            lh[h, :, :half] = high
            ll[h, :, :half] = low

    def cross(p):
        recv(half_copy, p, xp, me)
        along(p, xp)
        start(vir_copy(p, xp, 0, yp))

    def line(k, p, column, on=True, over=True):
        turned = p in TURNED and column == 0 and k <= TURN

        def act(offset, up):
            w = (me if column == 0 else xp) + offset
            if on:
                recv(vir_copy, p, w, 1, me)
                along(p, w, up, not up)
            if over and not turned:
                start(vir_copy(p, w, 0, yp))
        signs(k, act)

    def turn(k, p):
        if p not in TURNED or not TURN or k > TURN:
            return
        if k == 0:
            recv(vir_copy, p, yp, 0, me)
            along(p, yp)

        def act(offset, up):
            recv(vir_copy, p, yp + offset, 1, me)
            if k < TURN:
                along(p, yp + offset, up, not up)
        signs(k, act)

    def occ_wait():
        for d in range(nz):
            for other in (xp, yp, diag):
                occ_copy((other + 4 * d) % n, 0, me).wait_recv()

    def occ_join():
        for w in range(n):
            occ_dense[starts[w]:starts[w] + rows, :] += occ_all[w, :rows, :]
        oh[...], ol[...] = split(occ_dense[...].T[:, :half])

    def x_other():
        x_out[...] = product((oh[...], ol[...]), (lh[1 - core], ll[1 - core]))
        pair_copy().start()

    def x_mine():
        x_own[...] = product((oh[...], ol[...]), (lh[core], ll[core]))

    def x_start():
        pair_copy().wait_recv()
        x_send[...] = (x_own[...] + x_in[...]).reshape(x_send.shape)
        x_copy(mine, me, 0, xp).start()
        for d in range(1, npair):
            q = (mine + d) % npair
            x_copy(q, me, d, 2 * q + x).start()
        x_recv[me] = x_send[mine]

    def x_take(w):
        x_copy(mine, w, 0, me).wait_recv()
        x_pass(w, xp).start()

    orders = [sorted(range(nz), key=lambda other: (abs(other - zz), other)) for zz in range(nz)]

    def near(base, k):
        plane = 0
        for zz in range(nz):
            plane = plane + jnp.where(z == zz, orders[zz][k], 0)
        return base + 4 * (plane - z)

    def turns(line_base, other_base):
        order = sorted([(k, 0, line_base) for k in range(nz)] + [(k + 1.5, 1, other_base) for k in range(nz)], key=lambda e: e[:2])
        return [near(base, int(k - 1.5 * side)) for k, side, base in order]

    def x_relay(count):
        for w in relays[count[0]:count[1]]:
            x_take(w)

    relays = turns(me, yp)[1:]
    groups_of = [turns(me, yp)]
    passed = turns(xp, diag)
    groups_of += [passed[k:k + split_at] for k in range(0, len(passed), split_at)]

    def y_wait(p):
        for other in (yp, diag):
            first = TURN + 1 if p in TURNED and other is yp and TURN else 0
            if first == 0:
                recv(vir_copy, p, other, 0, me)
            for k in range(max(first, 1), nz):
                signs(k, lambda offset, up: recv(vir_copy, p, other + offset, 0, me))

    def join(w):
        top = starts[w]
        for t in range(full):
            dense[top:top + rows, t * LANES:(t + 1) * LANES] += va[w, t * rows:(t + 1) * rows, :]
        tail = va[w, body_rows:body_rows + 8, :]
        value = jnp.concatenate([pltpu.roll(tail, (LANES - g * rest) % LANES, 1) if g else tail for g in range(groups)], axis=0)
        value = jnp.where(lane < rest, value, 0)
        dense[top:top + rows, full * LANES:(full + 1) * LANES] += value[:rows]

    def join_side(mine_side):
        for yy in range(2):
            @pl.when((y == yy) == mine_side)
            def _():
                for w in range(n):
                    if (w // 2) % 2 == yy:
                        join(w)

    far = core != x

    def ready():
        high, low = split(dense[...])
        vh[...] = high
        vl[...] = low

    def chunk(g):
        group = groups_of[g]
        for w in group:
            if g:
                x_pass(w, me).wait_recv()
        rows_x = jnp.concatenate([x_recv[w] for w in group], axis=0)
        value = product(split(rows_x), (vh[...], vl[...]))
        for j, w in enumerate(group):
            low = value[j * block:j * block + block // 2]
            high = value[j * block + block // 2:(j + 1) * block]
            y_out[w] = jnp.where(core == 0, high, low)
            y_sum[w] = jnp.where(core == 0, low, high)
        for w in group:
            y_copy(w).start()

    def finish(g):
        for w in groups_of[g]:
            y_copy(w).wait_recv()
            total = y_sum[w] + y_in[w]
            y_sum[w] = total

            @pl.when(jnp.logical_not(far))
            def _():
                out_ref[w] = total[:, :wide]
        for w in groups_of[g]:
            pl.when(far)(lambda: o_copy(w).start())

    def last(g):
        for w in groups_of[g]:
            @pl.when(far)
            def _():
                o_copy(w).wait_recv()
                out_ref[w] = y_recv[w, :, :wide]

    pieces = range(len(parts))
    occ_start()
    for p in pieces:
        own_start(p)
    prepare()
    occ_line()
    for p in pieces:
        cross(p)
    for p in pieces:
        line(1, p, 0)
    for p in pieces:
        turn(0, p)
    occ_wait()
    occ_join()
    x_other()
    x_mine()
    for p in pieces:
        line(1, p, 1, over=False)
    for p in pieces:
        line(2, p, 0, over=False)
    x_start()
    for p in pieces:
        line(1, p, 1, on=False)
    for p in pieces:
        line(2, p, 0, on=False)
    for p in pieces:
        turn(1, p)
    for p in pieces:
        line(2, p, 1)
    x_relay((0, 1))
    for p in pieces:
        line(3, p, 0)
    for p in pieces:
        turn(2, p)
    x_relay((1, 2))
    for p in pieces:
        line(3, p, 1)
    for p in pieces:
        turn(3, p)
    x_relay((2, 2 * nz - 1))
    join_side(True)
    for p in pieces:
        y_wait(p)
    join_side(False)
    ready()
    chunk(0)
    for g in range(1, len(groups_of)):
        chunk(g)
        finish(g - 1)
    finish(len(groups_of) - 1)

    state["end"] = True
    occ_start()
    occ_line()
    for p in pieces:
        own_start(p)
        cross(p)
        for k in range(nz):
            line(k, p, 0)
            line(k, p, 1)
            turn(k, p)
    pair_copy().wait_send()
    for d in range(npair):
        x_copy(mine, me, d, xp).wait_send()
    for d in range(1, npair):
        x_pass(((2 * (mine + d)) % n) + x, xp).wait_send()
    for w in range(n):
        y_copy(w).wait_send()
        pl.when(far)(lambda: o_copy(w).wait_send())
    for g in list(range(1, len(groups_of))) + [0]:
        last(g)


def body(n, cholesky, coefficients):
    half, nao = cholesky.shape[1:]
    per = coefficients.shape[1]
    nmo = per * n // half
    nvir = nmo - NOCC
    sub = math.gcd(per, nmo)
    wide = nvir // 2
    full, rest = wide // LANES, wide % LANES
    starts = tuple(w * per // nmo for w in range(n))
    rows = max(-(-(w * per % nmo + per) // nmo) for w in range(n))
    deep = up_to(rows, 8)
    if cholesky.shape[0] != 1 or nmo != 2 * sub or rest == 0 or rest * (deep // 8) > LANES:
        return simple_body(cholesky, coefficients)
    tall = up_to(max(half, starts[-1] + rows), LANES)
    size = up_to(full * rows + 8, 8)
    cut = size // 16 * 8
    parts = ((0, cut), (cut, size - cut))
    iblock = NOCC // n
    spread = up_to(wide, LANES)
    nz = n // 4
    dma = pltpu.SemaphoreType.DMA
    vmem = pl.BlockSpec(memory_space=pltpu.VMEM)
    return pl.pallas_call(
        functools.partial(kernel, n, starts, rows, deep, sub, parts, GROUPS),
        out_shape=jax.ShapeDtypeStruct((n, iblock, wide), F32),
        in_specs=[vmem, pl.BlockSpec(memory_space=pl.ANY)],
        out_specs=vmem,
        scratch_shapes=[
            pltpu.VMEM((up_to(per // LANES + 2, 8), LANES), F32),
            pltpu.VMEM((up_to(sub, LANES) // LANES, up_to(9 + 2 * deep, 8), LANES), F32),
            pltpu.VMEM((n, deep, LANES), F32),
            pltpu.VMEM((size, LANES), F32),
            pltpu.VMEM((n, size, LANES), F32),
            pltpu.VMEM((half, nao), F32),
            pltpu.VMEM((2, half, tall), BF16),
            pltpu.VMEM((2, half, tall), BF16),
            pltpu.VMEM((tall, NOCC), F32),
            pltpu.VMEM((NOCC, half), BF16),
            pltpu.VMEM((NOCC, half), BF16),
            pltpu.VMEM((tall, spread), F32),
            pltpu.VMEM((tall, spread), BF16),
            pltpu.VMEM((tall, spread), BF16),
            pltpu.VMEM((NOCC, tall), F32),
            pltpu.VMEM((NOCC, tall), F32),
            pltpu.VMEM((NOCC, tall), F32),
            pltpu.VMEM((n // 2, 2 * iblock, tall), F32),
            pltpu.VMEM((n, 2 * iblock, tall), F32),
            *[pltpu.VMEM((n, iblock, spread), F32)] * 4,
            dma, dma((nz,)), dma((3, n)), dma((n,)), dma((len(parts),)), dma((3, len(parts), n)), dma((len(parts), n)),
            dma((n // 2,)), dma((n,)), dma((n,)), dma, dma, *[dma((n,))] * 4,
        ],
        compiler_params=pltpu.CompilerParams(
            collective_id=0, has_side_effects=True, vmem_limit_bytes=53 * 1024 * 1024),
        name="transform",
    )(coefficients, cholesky.reshape(half, nao))


def solution(mesh):
    n = mesh.shape["vec"]
    in_specs = (P("vec", "ao", None), P("ao", "vec"))
    out_specs = P(None, "vec", "ao")
    lines = n % 4 == 0 and mesh.shape["ao"] == 2 and NOCC % (8 * n) == 0
    step = functools.partial(body, n) if lines else simple_body
    return jax.shard_map(step, mesh=mesh, in_specs=in_specs, out_specs=out_specs, check_vma=False)
```

```python
import functools
import math

import jax
import jax.numpy as jnp
from jax import lax
from jax.experimental import pallas as pl
from jax.experimental.pallas import tpu as pltpu
from jax.sharding import PartitionSpec as P

NOCC = 128
LANES = 128
MESH = pl.DeviceIdType.MESH
F32 = jnp.float32
TURN, TURNED, GROUPS = 1, (1,), 4
BF16 = jnp.bfloat16


def up_to(size, step):
    return -(-size // step) * step


def simple_body(cholesky, coefficients):
    half_rows = cholesky.shape[1]
    own_flat = lax.all_gather(coefficients, "vec", axis=1, tiled=True)
    own_rows = own_flat.reshape(half_rows, own_flat.shape[1] // half_rows)
    occupied_own = own_rows[:, :NOCC]
    partial_x = jnp.einsum(
        "mi,pmn->pin",
        occupied_own,
        cholesky,
        precision=lax.Precision.HIGHEST,
        preferred_element_type=jnp.float32,
    )
    x_block = lax.psum_scatter(partial_x, "ao", scatter_dimension=2, tiled=True)
    virtual_own = own_rows[:, NOCC:]
    partial_y = jnp.einsum(
        "pin,na->pia",
        x_block,
        virtual_own,
        precision=lax.Precision.HIGHEST,
        preferred_element_type=jnp.float32,
    )
    summed = lax.psum_scatter(partial_y, "ao", scatter_dimension=2, tiled=True)
    owned = lax.all_to_all(summed, "vec", split_axis=1, concat_axis=0, tiled=True)
    return owned


def split(value):
    high = value.astype(BF16)
    return high, (value - high.astype(F32)).astype(BF16)


def product(left, right):
    (lh, ll), (rh, rl) = left, right
    dot = functools.partial(jnp.dot, preferred_element_type=F32)
    return dot(lh, rh) + (dot(lh, rl) + dot(ll, rh))


def tile_at(tiles, lane, offset):
    first, shift = divmod(offset, LANES)
    blank = jnp.zeros_like(tiles[0])
    here, after = (tiles[k] if 0 <= k < len(tiles) else blank for k in (first, first + 1))
    if shift == 0:
        return here
    turn = LANES - shift
    return jnp.where(lane < turn, pltpu.roll(here, turn, 1), pltpu.roll(after, turn, 1))


def kernel(
    n, starts, rows, deep, sub, parts, split_at, raw_ref, l_ref, out_ref,
    flat, sbuf, occ_all, vsend, va, l_buf, lh, ll, occ_dense, oh, ol, dense, vh, vl,
    x_out, x_in, x_own, x_send, x_recv, y_out, y_in, y_sum, y_recv, t_out, t_in,
    l_sem, occ_zs, occ_ss, occ_rs, vx_ss, v_ss, v_rs, x_ss, xf_ss, x_rs, pair_ss, pair_rs, y_ss, y_rs, o_ss, o_rs, t_ss, t_rs,
):
    me, core = lax.axis_index("vec"), lax.axis_index("ao")
    nz = n // 4
    x, y, z = me % 2, (me // 2) % 2, me // 4
    xp, yp, diag = me + 1 - 2 * x, me + 2 - 4 * y, me + 3 - 2 * x - 4 * y
    half, nao = l_ref.shape
    per = raw_ref.shape[1]
    subs = per // sub
    wide = out_ref.shape[2]
    full = wide // LANES
    rest = wide - full * LANES
    groups = deep // 8
    body_rows = full * rows
    block = 2 * out_ref.shape[1]
    npair = n // 2
    mine = me // 2

    l_copy = pltpu.make_async_copy(l_ref, l_buf, l_sem)
    l_copy.start()

    barrier = pltpu.get_barrier_semaphore()
    for to in [(me + 4 * d) % n for d in range(1, nz)] + [xp, yp, diag]:
        pl.semaphore_signal(barrier, inc=1, device_id=(to, core), device_id_type=MESH)
    pl.semaphore_signal(barrier, inc=1, device_id=(me, 1 - core), device_id_type=MESH)

    sbuf[...] = jnp.zeros_like(sbuf)
    for k in range(up_to(per, LANES) // LANES):
        width = min(LANES, per - k * LANES)
        flat[k:k + 1, :width] = raw_ref[:, k * LANES:k * LANES + width]
    period = LANES // math.gcd(sub, LANES)
    step = period * sub // LANES
    lane = lax.broadcasted_iota(jnp.int32, (deep, LANES), 1)
    for b in range(min(period, subs)):
        count = -(-(subs - b) // period)
        for t in range(sbuf.shape[0]):
            at, shift = divmod(b * sub + t * LANES, LANES)
            value = flat[pl.ds(at, count, stride=step), :]
            if shift:
                later = flat[pl.ds(at + 1, count, stride=step), :]
                turn = LANES - shift
                value = jnp.where(lane[:count] < turn, pltpu.roll(value, turn, 1), pltpu.roll(later, turn, 1))
            value = jnp.where(lane[:count] < sub - t * LANES, value, 0)
            sbuf[t, pl.ds(8 + b, count, stride=period), :] = value
    odd = (me * subs) % 2 == 1
    left, right = [], []
    for t in range(sbuf.shape[0]):
        before, even, after = (sbuf[t, pl.ds(8 + k, deep, stride=2), :] for k in (-1, 0, 1))
        left.append(jnp.where(odd, before, even))
        right.append(jnp.where(odd, even, after))
    columns = []
    for t in range(up_to(2 * sub, LANES) // LANES):
        value = tile_at(right, lane, t * LANES - sub)
        columns.append(value + left[t] if t < len(left) else value)
    occ_all[me] = columns[0]
    halves = [[tile_at(columns, lane, NOCC + h * wide + t * LANES) for t in range(full + 1)] for h in range(2)]
    tails = []
    for h in range(2):
        tail = jnp.zeros((8, LANES), F32)
        for g in range(groups):
            piece = jnp.where(lane[:8] < rest, halves[h][full][8 * g:8 * g + 8], 0)
            tail += pltpu.roll(piece, g * rest, 1) if g else piece
        tails.append(tail)
    for t in range(full):
        low, high = halves[0][t], halves[1][t]
        va[me, t * rows:(t + 1) * rows, :] = jnp.where(x == 0, low, high)[:rows]
        vsend[t * rows:(t + 1) * rows, :] = jnp.where(x == 0, high, low)[:rows]
    va[me, body_rows:body_rows + 8, :] = jnp.where(x == 0, tails[0], tails[1])
    vsend[body_rows:body_rows + 8, :] = jnp.where(x == 0, tails[1], tails[0])

    pl.semaphore_wait(barrier, nz + 3)

    def remote(src, dst, send_sem, recv_sem, to, on=core):
        return pltpu.make_async_remote_copy(
            src_ref=src, dst_ref=dst, send_sem=send_sem, recv_sem=recv_sem,
            device_id=(to, on), device_id_type=MESH)

    def occ_line_copy(w, d, to):
        return remote(occ_all.at[w], occ_all.at[w], occ_zs.at[d], occ_rs.at[w], to)

    def occ_copy(w, way, to):
        return remote(occ_all.at[w], occ_all.at[w], occ_ss.at[way, w], occ_rs.at[w], to)

    def half_copy(p, w, to):
        rng = pl.ds(parts[p][0], parts[p][1])
        return remote(vsend.at[rng], va.at[w, rng], vx_ss.at[p], v_rs.at[p, w], to)

    def vir_copy(p, w, way, to):
        ref = va.at[w, pl.ds(parts[p][0], parts[p][1])]
        return remote(ref, ref, v_ss.at[way, p, w], v_rs.at[p, w], to)

    def x_copy(q, w, d, to):
        return remote(x_send.at[q], x_recv.at[w], x_ss.at[d], x_rs.at[w], to)

    def x_pass(w, to):
        return remote(x_recv.at[w], x_recv.at[w], xf_ss.at[w], x_rs.at[w], to)

    def pair_copy():
        return remote(x_out, x_in, pair_ss, pair_rs, me, 1 - core)

    def y_copy(w):
        return remote(y_out.at[w], y_in.at[w], y_ss.at[w], y_rs.at[w], me, 1 - core)

    def o_copy(w):
        main = pl.ds(0, full * LANES)
        return remote(y_sum.at[w, :, main], y_recv.at[w, :, main], o_ss.at[w], o_rs.at[w], xp, 1 - core)

    def t_copy(slot):
        return remote(t_out.at[slot], t_in.at[slot], t_ss.at[slot], t_rs.at[slot], xp, 1 - core)

    state = dict(end=False)

    def start(copy):
        copy.wait_send() if state["end"] else copy.start()

    def recv(copy, *where):
        if not state["end"]:
            copy(*where).wait_recv()

    def signs(k, act):
        if 0 < k < nz:
            pl.when(z >= k)(lambda: act(-4 * k, True))
            pl.when(z + k < nz)(lambda: act(4 * k, False))

    def along(p, w, up=True, down=True):
        if up:
            pl.when(z < nz - 1)(lambda: start(vir_copy(p, w, 1, me + 4)))
        if down:
            pl.when(z > 0)(lambda: start(vir_copy(p, w, 2, me - 4)))

    def occ_spread(w):
        for way, to in enumerate((xp, yp, diag)):
            start(occ_copy(w, way, to))

    def occ_start():
        for d in range(1, nz):
            start(occ_line_copy(me, d, (me + 4 * d) % n))
        occ_spread(me)

    def occ_line():
        for k in range(1, nz):
            def act(offset, up):
                recv(occ_copy, me + offset, 0, me)
                occ_spread(me + offset)
            signs(k, act)

    def own_start(p):
        start(half_copy(p, me, xp))
        along(p, me)
        start(vir_copy(p, me, 0, yp))

    def prepare():
        dense[...] = jnp.zeros_like(dense)
        occ_dense[...] = jnp.zeros_like(occ_dense)
        edge = half // LANES * LANES
        lh[:, :, edge:] = jnp.zeros_like(lh[:, :, edge:])
        ll[:, :, edge:] = jnp.zeros_like(ll[:, :, edge:])
        l_copy.wait()
        for h in range(2):
            high, low = split(l_buf[:, h * half:(h + 1) * half])
            lh[h, :, :half] = high
            ll[h, :, :half] = low

    def cross(p):
        recv(half_copy, p, xp, me)
        along(p, xp)
        start(vir_copy(p, xp, 0, yp))

    def line(k, p, column, on=True, over=True):
        turned = p in TURNED and column == 0 and k <= TURN

        def act(offset, up):
            w = (me if column == 0 else xp) + offset
            if on:
                recv(vir_copy, p, w, 1, me)
                along(p, w, up, not up)
            if over and not turned:
                start(vir_copy(p, w, 0, yp))
        signs(k, act)

    def turn(k, p):
        if p not in TURNED or not TURN or k > TURN:
            return
        if k == 0:
            recv(vir_copy, p, yp, 0, me)
            along(p, yp)

        def act(offset, up):
            recv(vir_copy, p, yp + offset, 1, me)
            if k < TURN:
                along(p, yp + offset, up, not up)
        signs(k, act)

    def occ_wait(k):
        for other in (xp, yp, diag):
            if k == 0:
                occ_copy(other, 0, me).wait_recv()
            signs(k, lambda offset, up: occ_copy(other + offset, 0, me).wait_recv())

    def occ_join():
        for w in range(n):
            occ_dense[starts[w]:starts[w] + rows, :] += occ_all[w, :rows, :]
        oh[...], ol[...] = split(occ_dense[...].T[:, :half])

    def x_other():
        x_out[...] = product((oh[...], ol[...]), (lh[1 - core], ll[1 - core]))
        pair_copy().start()

    def x_mine():
        x_own[...] = product((oh[...], ol[...]), (lh[core], ll[core]))

    def x_start():
        pair_copy().wait_recv()
        x_send[...] = (x_own[...] + x_in[...]).reshape(x_send.shape)
        x_copy(mine, me, 0, xp).start()
        for d in range(1, npair):
            q = (mine + d) % npair
            x_copy(q, me, d, 2 * q + x).start()
        x_recv[me] = x_send[mine]

    def x_take(w):
        x_copy(mine, w, 0, me).wait_recv()
        x_pass(w, xp).start()

    orders = [sorted(range(nz), key=lambda other: (abs(other - zz), other)) for zz in range(nz)]

    def near(base, k):
        plane = 0
        for zz in range(nz):
            plane = plane + jnp.where(z == zz, orders[zz][k], 0)
        return base + 4 * (plane - z)

    def turns(line_base, other_base):
        order = sorted([(k, 0, line_base) for k in range(nz)] + [(k + 0.75, 1, other_base) for k in range(nz)], key=lambda e: e[:2])
        return [near(base, int(k - 0.75 * side)) for k, side, base in order]

    def x_relay(count):
        for w in relays[count[0]:count[1]]:
            x_take(w)

    relays = turns(me, yp)[1:]
    groups_of = [turns(me, yp)]
    passed = turns(xp, diag)
    groups_of += [passed[k:k + split_at] for k in range(0, len(passed), split_at)]

    def y_wait(p):
        for other in (yp, diag):
            first = TURN + 1 if p in TURNED and other is yp and TURN else 0
            if first == 0:
                recv(vir_copy, p, other, 0, me)
            for k in range(max(first, 1), nz):
                signs(k, lambda offset, up: recv(vir_copy, p, other + offset, 0, me))

    def join(w):
        top = starts[w]
        for t in range(full):
            dense[top:top + rows, t * LANES:(t + 1) * LANES] += va[w, t * rows:(t + 1) * rows, :]
        tail = va[w, body_rows:body_rows + 8, :]
        value = jnp.concatenate([pltpu.roll(tail, (LANES - g * rest) % LANES, 1) if g else tail for g in range(groups)], axis=0)
        value = jnp.where(lane < rest, value, 0)
        dense[top:top + rows, full * LANES:(full + 1) * LANES] += value[:rows]

    def join_side(mine_side):
        for yy in range(2):
            @pl.when((y == yy) == mine_side)
            def _():
                for w in range(n):
                    if (w // 2) % 2 == yy:
                        join(w)

    far = core != x

    def ready():
        high, low = split(dense[...])
        vh[...] = high
        vl[...] = low

    def chunk(g):
        group = groups_of[g]
        for w in group:
            if g:
                x_pass(w, me).wait_recv()
        rows_x = jnp.concatenate([x_recv[w] for w in group], axis=0)
        value = product(split(rows_x), (vh[...], vl[...]))
        for j, w in enumerate(group):
            low = value[j * block:j * block + block // 2]
            high = value[j * block + block // 2:(j + 1) * block]
            y_out[w] = jnp.where(core == 0, high, low)
            y_sum[w] = jnp.where(core == 0, low, high)
        for w in group:
            y_copy(w).start()

    def finish(g):
        for w in groups_of[g]:
            y_copy(w).wait_recv()
            total = y_sum[w] + y_in[w]
            y_sum[w] = total

            @pl.when(jnp.logical_not(far))
            def _():
                out_ref[w] = total[:, :wide]
        @pl.when(far)
        def _():
            for w in groups_of[g]:
                o_copy(w).start()
            for slot, packed in slots(groups_of, g):
                t_out[slot] = sum(pltpu.roll(y_sum[w, :, full * LANES:], j * rest, 1) if j else y_sum[w, :, full * LANES:] for j, w in enumerate(packed))
                t_copy(slot).start()

    def slots(groups, g):
        fit = LANES // rest
        base = sum(-(-len(group) // fit) for group in groups[:g])
        return [(base + k // fit, groups[g][k:k + fit]) for k in range(0, len(groups[g]), fit)]

    theirs = [turns(xp, diag)] + [turns(me, yp)[k:k + split_at] for k in range(0, n // 2, split_at)]

    def last(g):
        @pl.when(far)
        def _():
            for w in theirs[g]:
                o_copy(w).wait_recv()
                out_ref[w, :, :full * LANES] = y_recv[w, :, :full * LANES]
            for slot, packed in slots(theirs, g):
                t_copy(slot).wait_recv()
                tile = t_in[slot]
                for j, w in enumerate(packed):
                    out_ref[w, :, full * LANES:] = (pltpu.roll(tile, LANES - j * rest, 1) if j else tile)[:, :rest]

    pieces = range(len(parts))
    occ_start()
    for p in pieces:
        own_start(p)
    prepare()
    occ_line()
    for p in pieces:
        cross(p)
    for p in pieces:
        line(1, p, 0)
    for p in pieces:
        turn(0, p)
    occ_wait(0)
    occ_wait(1)
    occ_wait(2)
    for p in pieces:
        line(1, p, 1)
    occ_wait(3)
    occ_join()
    x_other()
    for p in pieces:
        line(2, p, 0, over=False)
    x_mine()
    x_start()
    for p in pieces:
        line(2, p, 0, on=False)
    for p in pieces:
        turn(1, p)
    for p in pieces:
        line(2, p, 1)
    for p in pieces:
        line(3, p, 0)
    x_relay((0, 4))
    for p in pieces:
        line(3, p, 1)
    x_relay((4, 2 * nz - 1))
    join_side(True)
    for p in pieces:
        y_wait(p)
    join_side(False)
    ready()
    chunk(0)
    for g in range(1, len(groups_of)):
        chunk(g)
        finish(g - 1)
    finish(len(groups_of) - 1)

    state["end"] = True
    occ_start()
    occ_line()
    for p in pieces:
        own_start(p)
        cross(p)
        for k in range(nz):
            line(k, p, 0)
            line(k, p, 1)
            turn(k, p)
    pair_copy().wait_send()
    for d in range(npair):
        x_copy(mine, me, d, xp).wait_send()
    for d in range(1, npair):
        x_pass(((2 * (mine + d)) % n) + x, xp).wait_send()
    for w in range(n):
        y_copy(w).wait_send()
        pl.when(far)(lambda: o_copy(w).wait_send())
    for g in range(len(theirs)):
        for slot, packed in slots(groups_of, g):
            pl.when(far)(lambda: t_copy(slot).wait_send())
        last(g)


def body(n, cholesky, coefficients):
    half, nao = cholesky.shape[1:]
    per = coefficients.shape[1]
    nmo = per * n // half
    nvir = nmo - NOCC
    sub = math.gcd(per, nmo)
    wide = nvir // 2
    full, rest = wide // LANES, wide % LANES
    starts = tuple(w * per // nmo for w in range(n))
    rows = max(-(-(w * per % nmo + per) // nmo) for w in range(n))
    deep = up_to(rows, 8)
    if cholesky.shape[0] != 1 or nmo != 2 * sub or rest == 0 or rest * (deep // 8) > LANES:
        return simple_body(cholesky, coefficients)
    tall = up_to(max(half, starts[-1] + rows), LANES)
    size = up_to(full * rows + 8, 8)
    cut = size // 16 * 8
    parts = ((0, cut), (cut, size - cut))
    iblock = NOCC // n
    spread = up_to(wide, LANES)
    nz = n // 4
    dma = pltpu.SemaphoreType.DMA
    vmem = pl.BlockSpec(memory_space=pltpu.VMEM)
    return pl.pallas_call(
        functools.partial(kernel, n, starts, rows, deep, sub, parts, GROUPS),
        out_shape=jax.ShapeDtypeStruct((n, iblock, wide), F32),
        in_specs=[vmem, pl.BlockSpec(memory_space=pl.ANY)],
        out_specs=vmem,
        scratch_shapes=[
            pltpu.VMEM((up_to(per // LANES + 2, 8), LANES), F32),
            pltpu.VMEM((up_to(sub, LANES) // LANES, up_to(9 + 2 * deep, 8), LANES), F32),
            pltpu.VMEM((n, deep, LANES), F32),
            pltpu.VMEM((size, LANES), F32),
            pltpu.VMEM((n, size, LANES), F32),
            pltpu.VMEM((half, nao), F32),
            pltpu.VMEM((2, half, tall), BF16),
            pltpu.VMEM((2, half, tall), BF16),
            pltpu.VMEM((tall, NOCC), F32),
            pltpu.VMEM((NOCC, half), BF16),
            pltpu.VMEM((NOCC, half), BF16),
            pltpu.VMEM((tall, spread), F32),
            pltpu.VMEM((tall, spread), BF16),
            pltpu.VMEM((tall, spread), BF16),
            pltpu.VMEM((NOCC, tall), F32),
            pltpu.VMEM((NOCC, tall), F32),
            pltpu.VMEM((NOCC, tall), F32),
            pltpu.VMEM((n // 2, 2 * iblock, tall), F32),
            pltpu.VMEM((n, 2 * iblock, tall), F32),
            *[pltpu.VMEM((n, iblock, spread), F32)] * 4,
            *[pltpu.VMEM((n, 8, LANES), F32)] * 2,
            dma, dma((nz,)), dma((3, n)), dma((n,)), dma((len(parts),)), dma((3, len(parts), n)), dma((len(parts), n)),
            dma((n // 2,)), dma((n,)), dma((n,)), dma, dma, *[dma((n,))] * 6,
        ],
        compiler_params=pltpu.CompilerParams(
            collective_id=0, has_side_effects=True, vmem_limit_bytes=53 * 1024 * 1024),
        name="transform",
    )(coefficients, cholesky.reshape(half, nao))


def solution(mesh):
    n = mesh.shape["vec"]
    in_specs = (P("vec", "ao", None), P("ao", "vec"))
    out_specs = P(None, "vec", "ao")
    lines = n % 4 == 0 and mesh.shape["ao"] == 2 and NOCC % (8 * n) == 0
    step = functools.partial(body, n) if lines else simple_body
    return jax.shard_map(step, mesh=mesh, in_specs=in_specs, out_specs=out_specs, check_vma=False)
```

```python
import functools
import math

import jax
import jax.numpy as jnp
from jax import lax
from jax.experimental import pallas as pl
from jax.experimental.pallas import tpu as pltpu
from jax.sharding import PartitionSpec as P

NOCC = 128
LANES = 128
MESH = pl.DeviceIdType.MESH
F32 = jnp.float32
TURN, TURNED, GROUPS = 1, (1,), 4
BF16 = jnp.bfloat16


def up_to(size, step):
    return -(-size // step) * step


def simple_body(cholesky, coefficients):
    half_rows = cholesky.shape[1]
    own_flat = lax.all_gather(coefficients, "vec", axis=1, tiled=True)
    own_rows = own_flat.reshape(half_rows, own_flat.shape[1] // half_rows)
    occupied_own = own_rows[:, :NOCC]
    partial_x = jnp.einsum(
        "mi,pmn->pin",
        occupied_own,
        cholesky,
        precision=lax.Precision.HIGHEST,
        preferred_element_type=jnp.float32,
    )
    x_block = lax.psum_scatter(partial_x, "ao", scatter_dimension=2, tiled=True)
    virtual_own = own_rows[:, NOCC:]
    partial_y = jnp.einsum(
        "pin,na->pia",
        x_block,
        virtual_own,
        precision=lax.Precision.HIGHEST,
        preferred_element_type=jnp.float32,
    )
    summed = lax.psum_scatter(partial_y, "ao", scatter_dimension=2, tiled=True)
    owned = lax.all_to_all(summed, "vec", split_axis=1, concat_axis=0, tiled=True)
    return owned


def split(value):
    high = value.astype(BF16)
    return high, (value - high.astype(F32)).astype(BF16)


def product(left, right):
    (lh, ll), (rh, rl) = left, right
    dot = functools.partial(jnp.dot, preferred_element_type=F32)
    return dot(lh, rh) + (dot(lh, rl) + dot(ll, rh))


def tile_at(tiles, lane, offset):
    first, shift = divmod(offset, LANES)
    blank = jnp.zeros_like(tiles[0])
    here, after = (tiles[k] if 0 <= k < len(tiles) else blank for k in (first, first + 1))
    if shift == 0:
        return here
    turn = LANES - shift
    return jnp.where(lane < turn, pltpu.roll(here, turn, 1), pltpu.roll(after, turn, 1))


def kernel(
    n, starts, rows, deep, sub, parts, split_at, raw_ref, l_ref, out_ref,
    flat, sbuf, occ_all, vsend, va, l_buf, lh, ll, occ_dense, oh, ol, dense, vh, vl,
    x_out, x_in, x_own, x_send, x_recv, y_out, y_in, y_sum, y_recv, t_out, t_in,
    l_sem, occ_zs, occ_ss, occ_rs, vx_ss, v_ss, v_rs, x_ss, xf_ss, x_rs, pair_ss, pair_rs, y_ss, y_rs, o_ss, o_rs, t_ss, t_rs,
):
    me, core = lax.axis_index("vec"), lax.axis_index("ao")
    nz = n // 4
    x, y, z = me % 2, (me // 2) % 2, me // 4
    xp, yp, diag = me + 1 - 2 * x, me + 2 - 4 * y, me + 3 - 2 * x - 4 * y
    half, nao = l_ref.shape
    per = raw_ref.shape[1]
    subs = per // sub
    wide = out_ref.shape[2]
    full = wide // LANES
    rest = wide - full * LANES
    groups = deep // 8
    body_rows = full * rows
    block = 2 * out_ref.shape[1]
    npair = n // 2
    mine = me // 2

    l_copy = pltpu.make_async_copy(l_ref, l_buf, l_sem)
    l_copy.start()

    barrier = pltpu.get_barrier_semaphore()
    for to in [(me + 4 * d) % n for d in range(1, nz)] + [xp, yp, diag]:
        pl.semaphore_signal(barrier, inc=1, device_id=(to, core), device_id_type=MESH)
    pl.semaphore_signal(barrier, inc=1, device_id=(me, 1 - core), device_id_type=MESH)

    sbuf[...] = jnp.zeros_like(sbuf)
    for k in range(up_to(per, LANES) // LANES):
        width = min(LANES, per - k * LANES)
        flat[k:k + 1, :width] = raw_ref[:, k * LANES:k * LANES + width]
    period = LANES // math.gcd(sub, LANES)
    step = period * sub // LANES
    lane = lax.broadcasted_iota(jnp.int32, (deep, LANES), 1)
    for b in range(min(period, subs)):
        count = -(-(subs - b) // period)
        for t in range(sbuf.shape[0]):
            at, shift = divmod(b * sub + t * LANES, LANES)
            value = flat[pl.ds(at, count, stride=step), :]
            if shift:
                later = flat[pl.ds(at + 1, count, stride=step), :]
                turn = LANES - shift
                value = jnp.where(lane[:count] < turn, pltpu.roll(value, turn, 1), pltpu.roll(later, turn, 1))
            value = jnp.where(lane[:count] < sub - t * LANES, value, 0)
            sbuf[t, pl.ds(8 + b, count, stride=period), :] = value
    odd = (me * subs) % 2 == 1
    left, right = [], []
    for t in range(sbuf.shape[0]):
        before, even, after = (sbuf[t, pl.ds(8 + k, deep, stride=2), :] for k in (-1, 0, 1))
        left.append(jnp.where(odd, before, even))
        right.append(jnp.where(odd, even, after))
    columns = []
    for t in range(up_to(2 * sub, LANES) // LANES):
        value = tile_at(right, lane, t * LANES - sub)
        columns.append(value + left[t] if t < len(left) else value)
    occ_all[me] = columns[0]
    halves = [[tile_at(columns, lane, NOCC + h * wide + t * LANES) for t in range(full + 1)] for h in range(2)]
    tails = []
    for h in range(2):
        tail = jnp.zeros((8, LANES), F32)
        for g in range(groups):
            piece = jnp.where(lane[:8] < rest, halves[h][full][8 * g:8 * g + 8], 0)
            tail += pltpu.roll(piece, g * rest, 1) if g else piece
        tails.append(tail)
    for t in range(full):
        low, high = halves[0][t], halves[1][t]
        va[me, t * rows:(t + 1) * rows, :] = jnp.where(x == 0, low, high)[:rows]
        vsend[t * rows:(t + 1) * rows, :] = jnp.where(x == 0, high, low)[:rows]
    va[me, body_rows:body_rows + 8, :] = jnp.where(x == 0, tails[0], tails[1])
    vsend[body_rows:body_rows + 8, :] = jnp.where(x == 0, tails[1], tails[0])

    pl.semaphore_wait(barrier, nz + 3)

    def remote(src, dst, send_sem, recv_sem, to, on=core):
        return pltpu.make_async_remote_copy(
            src_ref=src, dst_ref=dst, send_sem=send_sem, recv_sem=recv_sem,
            device_id=(to, on), device_id_type=MESH)

    def occ_line_copy(w, d, to):
        return remote(occ_all.at[w], occ_all.at[w], occ_zs.at[d], occ_rs.at[w], to)

    def occ_copy(w, way, to):
        return remote(occ_all.at[w], occ_all.at[w], occ_ss.at[way, w], occ_rs.at[w], to)

    def half_copy(p, w, to):
        rng = pl.ds(parts[p][0], parts[p][1])
        return remote(vsend.at[rng], va.at[w, rng], vx_ss.at[p], v_rs.at[p, w], to)

    def vir_copy(p, w, way, to):
        ref = va.at[w, pl.ds(parts[p][0], parts[p][1])]
        return remote(ref, ref, v_ss.at[way, p, w], v_rs.at[p, w], to)

    def x_copy(q, w, d, to):
        return remote(x_send.at[q], x_recv.at[w], x_ss.at[d], x_rs.at[w], to)

    def x_pass(w, to):
        return remote(x_recv.at[w], x_recv.at[w], xf_ss.at[w], x_rs.at[w], to)

    def pair_copy():
        return remote(x_out, x_in, pair_ss, pair_rs, me, 1 - core)

    def y_copy(w):
        return remote(y_out.at[w], y_in.at[w], y_ss.at[w], y_rs.at[w], me, 1 - core)

    def o_copy(w):
        main = pl.ds(0, full * LANES)
        return remote(y_sum.at[w, :, main], y_recv.at[w, :, main], o_ss.at[w], o_rs.at[w], xp, 1 - core)

    def t_copy(slot):
        return remote(t_out.at[slot], t_in.at[slot], t_ss.at[slot], t_rs.at[slot], xp, 1 - core)

    state = dict(end=False)

    def start(copy):
        copy.wait_send() if state["end"] else copy.start()

    def recv(copy, *where):
        if not state["end"]:
            copy(*where).wait_recv()

    def signs(k, act):
        if 0 < k < nz:
            pl.when(z >= k)(lambda: act(-4 * k, True))
            pl.when(z + k < nz)(lambda: act(4 * k, False))

    def along(p, w, up=True, down=True):
        if up:
            pl.when(z < nz - 1)(lambda: start(vir_copy(p, w, 1, me + 4)))
        if down:
            pl.when(z > 0)(lambda: start(vir_copy(p, w, 2, me - 4)))

    def occ_spread(w):
        for way, to in enumerate((xp, yp, diag)):
            start(occ_copy(w, way, to))

    def occ_start():
        for d in range(1, nz):
            start(occ_line_copy(me, d, (me + 4 * d) % n))
        occ_spread(me)

    def occ_line():
        for k in range(1, nz):
            def act(offset, up):
                recv(occ_copy, me + offset, 0, me)
                occ_spread(me + offset)
            signs(k, act)

    def own_start(p):
        start(half_copy(p, me, xp))
        along(p, me)
        start(vir_copy(p, me, 0, yp))

    def prepare():
        dense[...] = jnp.zeros_like(dense)
        occ_dense[...] = jnp.zeros_like(occ_dense)
        edge = half // LANES * LANES
        lh[:, :, edge:] = jnp.zeros_like(lh[:, :, edge:])
        ll[:, :, edge:] = jnp.zeros_like(ll[:, :, edge:])
        l_copy.wait()
        for h in range(2):
            high, low = split(l_buf[:, h * half:(h + 1) * half])
            lh[h, :, :half] = high
            ll[h, :, :half] = low

    def cross(p):
        recv(half_copy, p, xp, me)
        along(p, xp)
        start(vir_copy(p, xp, 0, yp))

    def line(k, p, column, on=True, over=True):
        turned = p in TURNED and column == 0 and k <= TURN

        def act(offset, up):
            w = (me if column == 0 else xp) + offset
            if on:
                recv(vir_copy, p, w, 1, me)
                along(p, w, up, not up)
            if over and not turned:
                start(vir_copy(p, w, 0, yp))
        signs(k, act)

    def turn(k, p):
        if p not in TURNED or not TURN or k > TURN:
            return
        if k == 0:
            recv(vir_copy, p, yp, 0, me)
            along(p, yp)

        def act(offset, up):
            recv(vir_copy, p, yp + offset, 1, me)
            if k < TURN:
                along(p, yp + offset, up, not up)
        signs(k, act)

    def occ_wait(k):
        for other in (xp, yp, diag):
            if k == 0:
                occ_copy(other, 0, me).wait_recv()
            signs(k, lambda offset, up: occ_copy(other + offset, 0, me).wait_recv())

    def occ_join():
        for w in range(n):
            occ_dense[starts[w]:starts[w] + rows, :] += occ_all[w, :rows, :]
        oh[...], ol[...] = split(occ_dense[...].T[:, :half])

    def x_other():
        x_out[...] = product((oh[...], ol[...]), (lh[1 - core], ll[1 - core]))
        pair_copy().start()

    def x_mine():
        x_own[...] = product((oh[...], ol[...]), (lh[core], ll[core]))

    def x_start():
        pair_copy().wait_recv()
        x_send[...] = (x_own[...] + x_in[...]).reshape(x_send.shape)
        x_copy(mine, me, 0, xp).start()
        for d in range(1, npair):
            q = (mine + d) % npair
            x_copy(q, me, d, 2 * q + x).start()
        x_recv[me] = x_send[mine]

    def x_take(w):
        x_copy(mine, w, 0, me).wait_recv()
        x_pass(w, xp).start()

    orders = [sorted(range(nz), key=lambda other: (abs(other - zz), other)) for zz in range(nz)]

    def near(base, k):
        plane = 0
        for zz in range(nz):
            plane = plane + jnp.where(z == zz, orders[zz][k], 0)
        return base + 4 * (plane - z)

    def turns(line_base, other_base):
        order = sorted([(k, 0, line_base) for k in range(nz)] + [(k + 0.75, 1, other_base) for k in range(nz)], key=lambda e: e[:2])
        return [near(base, int(k - 0.75 * side)) for k, side, base in order]

    def x_relay(count):
        for w in relays[count[0]:count[1]]:
            x_take(w)

    relays = turns(me, yp)[1:]
    groups_of = [turns(me, yp)]
    passed = turns(xp, diag)
    groups_of += [passed[k:k + split_at] for k in range(0, len(passed), split_at)]

    def y_wait(p):
        for other in (yp, diag):
            first = TURN + 1 if p in TURNED and other is yp and TURN else 0
            if first == 0:
                recv(vir_copy, p, other, 0, me)
            for k in range(max(first, 1), nz):
                signs(k, lambda offset, up: recv(vir_copy, p, other + offset, 0, me))

    early = parts[0][1] // rows
    edge = early * LANES

    def join(w, first):
        top = starts[w]
        for t in range(early) if first else range(early, full):
            dense[top:top + rows, t * LANES:(t + 1) * LANES] += va[w, t * rows:(t + 1) * rows, :]
        if first:
            return
        tail = va[w, body_rows:body_rows + 8, :]
        value = jnp.concatenate([pltpu.roll(tail, (LANES - g * rest) % LANES, 1) if g else tail for g in range(groups)], axis=0)
        value = jnp.where(lane < rest, value, 0)
        dense[top:top + rows, full * LANES:(full + 1) * LANES] += value[:rows]

    def join_side(mine_side, first):
        for yy in range(2):
            @pl.when((y == yy) == mine_side)
            def _():
                for w in range(n):
                    if (w // 2) % 2 == yy:
                        join(w, first)

    far = core != x

    def ready(first):
        where = slice(0, edge) if first else slice(edge, dense.shape[1])
        high, low = split(dense[:, where])
        vh[:, where] = high
        vl[:, where] = low

    def columns_of(g, where):
        rows_x = jnp.concatenate([x_recv[w] for w in groups_of[g]], axis=0)
        return product(split(rows_x), (vh[:, where], vl[:, where]))

    def chunk(g, before=None):
        group = groups_of[g]
        for w in group:
            if g:
                x_pass(w, me).wait_recv()
        if before is None:
            value = columns_of(g, slice(0, dense.shape[1]))
        else:
            value = jnp.concatenate([before, columns_of(g, slice(edge, dense.shape[1]))], axis=1)
        for j, w in enumerate(group):
            low = value[j * block:j * block + block // 2]
            high = value[j * block + block // 2:(j + 1) * block]
            y_out[w] = jnp.where(core == 0, high, low)
            y_sum[w] = jnp.where(core == 0, low, high)
        for w in group:
            y_copy(w).start()

    def finish(g):
        for w in groups_of[g]:
            y_copy(w).wait_recv()
            total = y_sum[w] + y_in[w]
            y_sum[w] = total

            @pl.when(jnp.logical_not(far))
            def _():
                out_ref[w] = total[:, :wide]
        @pl.when(far)
        def _():
            for w in groups_of[g]:
                o_copy(w).start()
            for slot, packed in slots(groups_of, g):
                t_out[slot] = sum(pltpu.roll(y_sum[w, :, full * LANES:], j * rest, 1) if j else y_sum[w, :, full * LANES:] for j, w in enumerate(packed))
                t_copy(slot).start()

    def slots(groups, g):
        fit = LANES // rest
        base = sum(-(-len(group) // fit) for group in groups[:g])
        return [(base + k // fit, groups[g][k:k + fit]) for k in range(0, len(groups[g]), fit)]

    theirs = [turns(xp, diag)] + [turns(me, yp)[k:k + split_at] for k in range(0, n // 2, split_at)]

    def last(g):
        @pl.when(far)
        def _():
            for w in theirs[g]:
                o_copy(w).wait_recv()
                out_ref[w, :, :full * LANES] = y_recv[w, :, :full * LANES]
            for slot, packed in slots(theirs, g):
                t_copy(slot).wait_recv()
                tile = t_in[slot]
                for j, w in enumerate(packed):
                    out_ref[w, :, full * LANES:] = (pltpu.roll(tile, LANES - j * rest, 1) if j else tile)[:, :rest]

    pieces = range(len(parts))
    occ_start()
    for p in pieces:
        own_start(p)
    prepare()
    occ_line()
    for p in pieces:
        cross(p)
    for p in pieces:
        line(1, p, 0)
    for p in pieces:
        turn(0, p)
    occ_wait(0)
    occ_wait(1)
    occ_wait(2)
    for p in pieces:
        line(1, p, 1)
    occ_wait(3)
    occ_join()
    x_other()
    for p in pieces:
        line(2, p, 0, over=False)
    x_mine()
    x_start()
    for p in pieces:
        line(2, p, 0, on=False)
    for p in pieces:
        turn(1, p)
    for p in pieces:
        line(2, p, 1)
    for p in pieces:
        line(3, p, 0)
    x_relay((0, 4))
    for p in pieces:
        line(3, p, 1)
    x_relay((4, 2 * nz - 1))
    join_side(True, True)
    join_side(True, False)
    y_wait(0)
    join_side(False, True)
    ready(True)
    before = columns_of(0, slice(0, edge))
    for p in pieces[1:]:
        y_wait(p)
    join_side(False, False)
    ready(False)
    chunk(0, before)
    for g in range(1, len(groups_of)):
        chunk(g)
        finish(g - 1)
    finish(len(groups_of) - 1)

    state["end"] = True
    occ_start()
    occ_line()
    for p in pieces:
        own_start(p)
        cross(p)
        for k in range(nz):
            line(k, p, 0)
            line(k, p, 1)
            turn(k, p)
    pair_copy().wait_send()
    for d in range(npair):
        x_copy(mine, me, d, xp).wait_send()
    for d in range(1, npair):
        x_pass(((2 * (mine + d)) % n) + x, xp).wait_send()
    for w in range(n):
        y_copy(w).wait_send()
        pl.when(far)(lambda: o_copy(w).wait_send())
    for g in range(len(theirs)):
        for slot, packed in slots(groups_of, g):
            pl.when(far)(lambda: t_copy(slot).wait_send())
        last(g)


def body(n, cholesky, coefficients):
    half, nao = cholesky.shape[1:]
    per = coefficients.shape[1]
    nmo = per * n // half
    nvir = nmo - NOCC
    sub = math.gcd(per, nmo)
    wide = nvir // 2
    full, rest = wide // LANES, wide % LANES
    starts = tuple(w * per // nmo for w in range(n))
    rows = max(-(-(w * per % nmo + per) // nmo) for w in range(n))
    deep = up_to(rows, 8)
    if cholesky.shape[0] != 1 or nmo != 2 * sub or rest == 0 or rest * (deep // 8) > LANES:
        return simple_body(cholesky, coefficients)
    tall = up_to(max(half, starts[-1] + rows), LANES)
    size = up_to(full * rows + 8, 8)
    cut = size // 16 * 8
    parts = ((0, cut), (cut, size - cut))
    iblock = NOCC // n
    spread = up_to(wide, LANES)
    nz = n // 4
    dma = pltpu.SemaphoreType.DMA
    vmem = pl.BlockSpec(memory_space=pltpu.VMEM)
    return pl.pallas_call(
        functools.partial(kernel, n, starts, rows, deep, sub, parts, GROUPS),
        out_shape=jax.ShapeDtypeStruct((n, iblock, wide), F32),
        in_specs=[vmem, pl.BlockSpec(memory_space=pl.ANY)],
        out_specs=vmem,
        scratch_shapes=[
            pltpu.VMEM((up_to(per // LANES + 2, 8), LANES), F32),
            pltpu.VMEM((up_to(sub, LANES) // LANES, up_to(9 + 2 * deep, 8), LANES), F32),
            pltpu.VMEM((n, deep, LANES), F32),
            pltpu.VMEM((size, LANES), F32),
            pltpu.VMEM((n, size, LANES), F32),
            pltpu.VMEM((half, nao), F32),
            pltpu.VMEM((2, half, tall), BF16),
            pltpu.VMEM((2, half, tall), BF16),
            pltpu.VMEM((tall, NOCC), F32),
            pltpu.VMEM((NOCC, half), BF16),
            pltpu.VMEM((NOCC, half), BF16),
            pltpu.VMEM((tall, spread), F32),
            pltpu.VMEM((tall, spread), BF16),
            pltpu.VMEM((tall, spread), BF16),
            pltpu.VMEM((NOCC, tall), F32),
            pltpu.VMEM((NOCC, tall), F32),
            pltpu.VMEM((NOCC, tall), F32),
            pltpu.VMEM((n // 2, 2 * iblock, tall), F32),
            pltpu.VMEM((n, 2 * iblock, tall), F32),
            *[pltpu.VMEM((n, iblock, spread), F32)] * 4,
            *[pltpu.VMEM((n, 8, LANES), F32)] * 2,
            dma, dma((nz,)), dma((3, n)), dma((n,)), dma((len(parts),)), dma((3, len(parts), n)), dma((len(parts), n)),
            dma((n // 2,)), dma((n,)), dma((n,)), dma, dma, *[dma((n,))] * 6,
        ],
        compiler_params=pltpu.CompilerParams(
            collective_id=0, has_side_effects=True, vmem_limit_bytes=53 * 1024 * 1024),
        name="transform",
    )(coefficients, cholesky.reshape(half, nao))


def solution(mesh):
    n = mesh.shape["vec"]
    in_specs = (P("vec", "ao", None), P("ao", "vec"))
    out_specs = P(None, "vec", "ao")
    lines = n % 4 == 0 and mesh.shape["ao"] == 2 and NOCC % (8 * n) == 0
    step = functools.partial(body, n) if lines else simple_body
    return jax.shard_map(step, mesh=mesh, in_specs=in_specs, out_specs=out_specs, check_vma=False)
```
